512 devices in a mesh: prow: 16 (over z), pcol: 32 (over x, y, core).
Axes of the slice: x: 4, y: 4, z: 16, core: 2. Of those that a mesh axis runs over, the one named last changes fastest.
Arguments:
- matrix: float32 [8192, 32768], P('prow', 'pcol'), may hold values from -6 to 6
- pivot_inverse: float32 [2, 512, 512], P(None, 'prow'), may hold values from -0.01171875 to 0.01171875
- row_live: int32 [2, 16], replicated, may hold values 0 or 1
- col_live: int32 [2, 64], replicated, may hold values 0 or 1
Outputs:
- factored: float32 [8192, 32768], P('prow', 'pcol')
The draws below stay inside these ranges and needn't reach their ends.
All inputs are finite; a program needn't handle non-finite values.
Results may differ from the reference program's by a relative error of at most 0.0001.
Values sent between devices are 32-bit elements; how exact they have to be, the bound alone decides.
No kernel may reach another device: no remote copies, remote signals or barrier semaphores. Data moves between devices by JAX's collectives and lax.ppermute only.
A program may use at most 64 MiB of HBM per device.

```python
import jax
import jax.numpy as jnp
from jax import lax

B = 512
RB = 1
CB = 2
PANELS = 2
NBR = 16
NBC = 64
N_PROW = 16
N_PCOL = 32


def plant(result, key, least, high):
    shape = result.shape
    index_at = [jax.random.randint(jax.random.fold_in(key, axis), (), 0, shape[axis]) for axis in range(len(shape))]
    result = result.at[tuple(index_at)].set(least)
    longest = shape.index(max(shape))
    index_at[longest] = (index_at[longest] + 1) % shape[longest]
    return result.at[tuple(index_at)].set(high)


def levels(rng, dims, shards, least, high):
    def one(dim, shards_of):
        draws = jax.random.uniform(jax.random.fold_in(jax.random.fold_in(rng, 6), dim), (shards_of,), jnp.float32, least / len(shards), high / len(shards))
        return jnp.repeat(jnp.exp(draws), dims[dim] // shards_of).reshape((-1,) + (1,) * (len(dims) - dim - 1))

    level = one(*shards[0])
    for cut in shards[1:]:
        level = level * one(*cut)
    return level


def noise(rng, extent, deviation, bound, shards=(), held_as=jnp.bfloat16):
    values = deviation * jax.random.normal(rng, extent, jnp.float32)
    if shards:
        values = values * levels(rng, extent, shards, -0.22, 0.18)
    return jnp.clip(values, -bound, bound).astype(held_as)


def setup_inputs(seed: int = 0) -> dict:
    seeds = jax.random.split(jax.random.key(seed), 5)
    matrix = noise(seeds[0], (NBR * B, NBC * B), 1.0, 6.0, ((0, 16), (1, 32)), jnp.float32)
    pivot_inverse = noise(seeds[1], (PANELS, B, B), (B * B) ** -0.5, 0.01171875, ((1, 16),), jnp.float32)
    row_live = plant((jax.random.randint(seeds[2], (PANELS, NBR), 0, 4) < 3).astype(jnp.int32), jax.random.fold_in(seeds[2], 1), 0, 1)
    col_live = plant((jax.random.randint(seeds[3], (PANELS, NBC), 0, 4) < 3).astype(jnp.int32), jax.random.fold_in(seeds[3], 1), 0, 1)
    return dict(matrix=matrix, pivot_inverse=pivot_inverse, row_live=row_live, col_live=col_live)


def reference(matrix, pivot_inverse, row_live, col_live):
    block_rows = RB * N_PROW
    block_cols = CB * N_PCOL
    row_range = jnp.arange(block_rows, dtype=jnp.int32)
    col_range = jnp.arange(block_cols, dtype=jnp.int32)
    row_index = (row_range % RB) * N_PROW + row_range // RB
    col_index = (col_range % CB) * N_PCOL + col_range // CB
    for panel in range(PANELS):
        lower_mask = jnp.where(row_index > panel, jnp.take(row_live[panel], row_index), 0).astype(jnp.float32)
        upper_mask = jnp.where(col_index > panel, jnp.take(col_live[panel], col_index), 0).astype(jnp.float32)
        lower_mask = jnp.repeat(lower_mask, B)
        upper_mask = jnp.repeat(upper_mask, B)
        col_start = panel * CB * B
        row_start = panel * RB * B
        column_part = matrix[:, col_start:col_start + B]
        lower_part = jnp.dot(column_part, pivot_inverse[panel], precision=lax.Precision.HIGHEST) * lower_mask[:, None]
        upper_part = matrix[row_start:row_start + B, :] * upper_mask[None, :]
        matrix = matrix - jnp.dot(lower_part, upper_part, precision=lax.Precision.HIGHEST)
        keep_rows = jnp.repeat(row_index > panel, B)[:, None]
        matrix = matrix.at[:, col_start:col_start + B].set(jnp.where(keep_rows, lower_part, matrix[:, col_start:col_start + B]))
    return matrix
```

```python
import jax
import jax.numpy as jnp
from jax import lax
from jax.sharding import PartitionSpec as P


ROWS, COLS = "prow", "pcol"
TILE = 8


def matmul(a, b):
    return jnp.dot(a, b, precision=lax.Precision.HIGH)


def exchange(pieces, axis, groups=None):
    return lax.all_to_all(
        pieces, axis, split_axis=0, concat_axis=0, tiled=True, axis_index_groups=groups
    )


def copies(piece, count):
    return jnp.broadcast_to(piece, (count, *piece.shape))


def send_order(count):
    half = [d for i in range(1, count // 2) for d in (i, count - i)]
    return [count // 2, *reversed(half)]


def scatter_rows(matrix):
    count, here = lax.axis_size(ROWS), lax.axis_index(ROWS)
    length = matrix.shape[0] // count
    turned = jnp.where(here == 1, jnp.roll(matrix, -length, axis=0), matrix)
    first = second = turned[:length]
    for d in send_order(count):
        pairs = [(0, d), (1, (1 + d) % count)]
        came = lax.ppermute(turned[d * length : (d + 1) * length], ROWS, pairs)
        first = jnp.where(here == d, came, first)
        second = jnp.where(here == (1 + d) % count, came, second)
    return jnp.concatenate([first, second], axis=0)


def plane(count):
    side = round((count // 2) ** 0.5)
    return side, lambda x, y, core: (x * side + y) * 2 + core


def holders(blocks):
    count = blocks.shape[0]
    side, _ = plane(count)
    grid = blocks.reshape(2, side, side, *blocks.shape[1:])
    both = jnp.stack([jnp.swapaxes(grid[0], 0, 1), grid[1]], axis=2)
    return both.reshape(blocks.shape)


def gather_plane(piece):
    count, core = lax.axis_size(COLS), lax.axis_index(COLS) % 2
    side, at = plane(count)
    span = range(side)
    along_x = [[[at(x, y, c) for x in span] for y in span] for c in (0, 1)]
    along_y = [[[at(x, y, c) for y in span] for x in span] for c in (0, 1)]
    part = exchange(copies(piece, side), COLS, along_x[0] + along_y[1])
    part = exchange(copies(part, side), COLS, along_y[0] + along_x[1])
    part = part.reshape(side * side, *piece.shape)
    other = lax.ppermute(part, COLS, [(i, i ^ 1) for i in range(count)])
    low, high = jnp.where(core == 0, part, other), jnp.where(core == 0, other, part)
    return jnp.concatenate([low, high], axis=0)


def per_device(matrix, pivot_inverse, row_live, col_live):
    width = pivot_inverse.shape[2]
    n_rows, n_cols = lax.axis_size(ROWS), lax.axis_size(COLS)
    g, p = lax.axis_index(ROWS), lax.axis_index(COLS)
    lines = width // n_cols
    lane = width * 2 * pivot_inverse.shape[1] // (TILE * n_cols)
    row_groups, col_groups = pivot_inverse.shape[1] // TILE, width // lane

    spread = exchange(holders(matrix[:, :width].reshape(n_cols, lines, width)), COLS)
    mine = spread[:2]

    raw = lax.all_gather(scatter_rows(matrix), ROWS, axis=0, tiled=True)
    raw = raw.reshape(n_rows, 2, -1, matrix.shape[1])
    raw0, raw1 = raw[:, 0].reshape(matrix.shape), raw[:, 1].reshape(matrix.shape)

    sent = jnp.where(g == 0, mine[1], mine[0]).reshape(n_rows, lines // n_rows, width)
    got = exchange(sent, ROWS)[:2]
    tiles = pivot_inverse.reshape(2, row_groups, TILE, col_groups, lane)
    tiles = tiles.transpose(0, 1, 3, 2, 4).reshape(n_cols, TILE, lane)
    tile = lax.dynamic_index_in_dim(holders(tiles), p, keepdims=False)
    small = jnp.concatenate([got.reshape(-1, lane), tile], axis=0)
    split = got.size // lane
    small = exchange(copies(small, n_rows), ROWS)
    cross = small[:, :split].reshape(n_rows, 2, lines // n_rows, width)
    cross = cross.transpose(1, 0, 2, 3).reshape(2 * lines, width)
    wide = width // lane
    pivots = small[:, split:].reshape(n_rows // wide, wide, TILE, lane)
    pivots = pivots.transpose(0, 2, 1, 3).reshape(-1, width)

    piece = jnp.concatenate([mine.reshape(2 * lines, width), cross, pivots], axis=0)
    shared = gather_plane(piece)
    a_g0, a_g1, a_01, a_10 = (
        shared[:, i * lines : (i + 1) * lines].reshape(width, width) for i in range(4)
    )
    inverse = shared[:, 4 * lines :].reshape(
        2, row_groups, col_groups, n_rows // wide, TILE, wide, lane
    )
    inverse = inverse.transpose(0, 3, 5, 1, 4, 2, 6).reshape(2, width, width)

    def lower(panel, row):
        return jnp.where(row > panel, row_live[panel, row], 0).astype(jnp.float32)

    col_index = jnp.arange(matrix.shape[1] // width, dtype=jnp.int32) * n_cols + p

    def upper(panel):
        live = jnp.where(col_index > panel, jnp.take(col_live[panel], col_index), 0)
        return live.astype(jnp.float32)

    up0, up1 = upper(0), upper(1)
    both = matmul(jnp.concatenate([a_g0, a_10], axis=0), inverse[0])
    lower0 = both[:width] * lower(0, g)
    pivot_lower = both[width:] * lower(0, jnp.int32(1))
    a_g1 = a_g1 - matmul(lower0, a_01 * col_live[0, 1].astype(jnp.float32))
    lower1 = matmul(a_g1, inverse[1]) * lower(1, g)
    mixed = matmul(lower1, pivot_lower)

    out = []
    for j in range(matrix.shape[1] // width):
        span = slice(j * width, (j + 1) * width)
        left0 = (lower0 - mixed * up1[j]) * up0[j]
        block = matrix[:, span] - matmul(left0, raw0[:, span])
        block = block - matmul(lower1 * up1[j], raw1[:, span])
        if j == 0:
            block = jnp.where((p == 0) & (g > 0), lower0, block)
            block = jnp.where((p == 1) & (g > 1), lower1, block)
        out.append(block)
    return jnp.concatenate(out, axis=1)


def solution(mesh):
    in_specs = (P(ROWS, COLS), P(None, ROWS, None), P(), P())
    return jax.shard_map(
        per_device, mesh=mesh, in_specs=in_specs, out_specs=P(ROWS, COLS), check_vma=False
    )
```

```python
import functools

import jax
import jax.numpy as jnp
from jax import lax
from jax.experimental import pallas as pl
from jax.experimental.pallas import tpu as pltpu
from jax.sharding import PartitionSpec as P


ROWS, COLS = "prow", "pcol"
TILE = 8


def matmul(a, b):
    return jnp.dot(a, b, precision=lax.Precision.HIGH)


def exchange(pieces, axis, groups=None):
    return lax.all_to_all(
        pieces, axis, split_axis=0, concat_axis=0, tiled=True, axis_index_groups=groups
    )


def copies(piece, count):
    return jnp.broadcast_to(piece, (count, *piece.shape))


def send_order(count):
    half = [d for i in range(1, count // 2) for d in (i, count - i)]
    return [*half, count // 2]


def scatter_rows(matrix):
    count, here = lax.axis_size(ROWS), lax.axis_index(ROWS)
    length = matrix.shape[0] // count
    turned = jnp.where(here == 1, jnp.roll(matrix, -length, axis=0), matrix)
    first = second = turned[:length]
    for d in send_order(count):
        pairs = [(0, d), (1, (1 + d) % count)]
        came = lax.ppermute(turned[d * length : (d + 1) * length], ROWS, pairs)
        first = jnp.where(here == d, came, first)
        second = jnp.where(here == (1 + d) % count, came, second)
    return jnp.concatenate([first, second], axis=0)


def tree_copies(own):
    count, here = lax.axis_size(ROWS), lax.axis_index(ROWS)
    held = own
    for c in range(4, count, 4):
        came = lax.ppermute(own, ROWS, [(0, c), (1, c + 1)])
        held = jnp.where((here == c) | (here == c + 1), came, held)
    leaves = [held]
    for step in (1, 2, -1):
        pairs = [((c + k) % count, (c + k + step) % count) for c in range(0, count, 4) for k in (0, 1)]
        leaves.append(lax.ppermute(held, ROWS, pairs))

    def of(place):
        found = leaves[0]
        for i in (1, 2, 3):
            found = jnp.where(place % 4 == i, leaves[i], found)
        return found

    return of(here), of(here + 3)


def plane(count):
    side = round((count // 2) ** 0.5)
    return side, lambda x, y, core: (x * side + y) * 2 + core


def holders(blocks):
    count = blocks.shape[0]
    side, _ = plane(count)
    grid = blocks.reshape(2, side, side, *blocks.shape[1:])
    both = jnp.stack([jnp.swapaxes(grid[0], 0, 1), grid[1]], axis=2)
    return both.reshape(blocks.shape)


def gather_plane(piece):
    count, core = lax.axis_size(COLS), lax.axis_index(COLS) % 2
    side, at = plane(count)
    span = range(side)
    along_x = [[[at(x, y, c) for x in span] for y in span] for c in (0, 1)]
    along_y = [[[at(x, y, c) for y in span] for x in span] for c in (0, 1)]
    part = exchange(copies(piece, side), COLS, along_x[0] + along_y[1])
    part = exchange(copies(part, side), COLS, along_y[0] + along_x[1])
    part = part.reshape(side * side, *piece.shape)
    other = lax.ppermute(part, COLS, [(i, i ^ 1) for i in range(count)])
    low, high = jnp.where(core == 0, part, other), jnp.where(core == 0, other, part)
    return jnp.concatenate([low, high], axis=0)


def halves(x):
    high = x.astype(jnp.bfloat16)
    return high, (x - high.astype(jnp.float32)).astype(jnp.bfloat16)


def update_kernel(steps, length, keeps, matrix, raw, left, stored, out, high, low):
    step = pl.program_id(0)

    @pl.when(step % steps == 0)
    def _():
        high[...], low[...] = halves(left[0])

    rows = raw.shape[0]
    starts = [*range(0, rows, 2 * length), *range(length, rows, 2 * length)]
    split = [jnp.concatenate([x[i : i + length] for i in starts]) for x in halves(raw[...])]
    dot = functools.partial(jnp.dot, preferred_element_type=jnp.float32)
    product = dot(high[...], split[0]) + (dot(high[...], split[1]) + dot(low[...], split[0]))
    new = matrix[...] - product
    out[...] = jnp.where((keeps[0] == 1) & (step < steps), stored[...], new)


def update(keeps, matrix, raw, left, stored, length):
    rows, width = stored.shape
    cols = matrix.shape[1]
    wide = min(256, width)
    steps = width // wide
    return pl.pallas_call(
        functools.partial(update_kernel, steps, length),
        grid_spec=pltpu.PrefetchScalarGridSpec(
            num_scalar_prefetch=1,
            grid=(cols // wide,),
            in_specs=[
                pl.BlockSpec((rows, wide), lambda t, _: (0, t)),
                pl.BlockSpec((2 * rows, wide), lambda t, _: (0, t)),
                pl.BlockSpec((1, rows, 2 * rows), lambda t, _: (t // steps, 0, 0)),
                pl.BlockSpec((rows, wide), lambda t, _: (0, jnp.minimum(t, steps - 1))),
            ],
            out_specs=pl.BlockSpec((rows, wide), lambda t, _: (0, t)),
            scratch_shapes=[pltpu.VMEM((rows, 2 * rows), jnp.bfloat16)] * 2,
        ),
        out_shape=jax.ShapeDtypeStruct(matrix.shape, jnp.float32),
        cost_estimate=pl.CostEstimate(
            flops=12 * rows * rows * cols, bytes_accessed=32 * rows * cols, transcendentals=0
        ),
        name="update",
    )(keeps, matrix, raw, left, stored)


def per_device(matrix, pivot_inverse, row_live, col_live):
    width = pivot_inverse.shape[2]
    n_rows, n_cols = lax.axis_size(ROWS), lax.axis_size(COLS)
    g, p = lax.axis_index(ROWS), lax.axis_index(COLS)
    lines = width // n_cols
    lane = width * 2 * pivot_inverse.shape[1] // (TILE * n_cols)
    row_groups, col_groups = pivot_inverse.shape[1] // TILE, width // lane

    spread = exchange(holders(matrix[:, :width].reshape(n_cols, lines, width)), COLS)
    mine = spread[:2]

    pieces = scatter_rows(matrix)
    raw = lax.all_gather(pieces, ROWS, axis=0, tiled=True)

    cross = tree_copies(jnp.where(g == 0, mine[1], mine[0]))
    tiles = pivot_inverse.reshape(2, row_groups, TILE, col_groups, lane)
    tiles = tiles.transpose(0, 1, 3, 2, 4).reshape(n_cols, TILE, lane)
    tile = lax.dynamic_index_in_dim(holders(tiles), p, keepdims=False)
    pivots = exchange(copies(tile, n_rows), ROWS)
    wide = width // lane
    pivots = pivots.reshape(n_rows // wide, wide, TILE, lane)
    pivots = pivots.transpose(0, 2, 1, 3).reshape(-1, width)

    piece = jnp.concatenate([*mine, *cross, pivots], axis=0)
    shared = gather_plane(piece)
    a_g0, a_g1, a_01, a_10 = (
        shared[:, i * lines : (i + 1) * lines].reshape(width, width) for i in range(4)
    )
    inverse = shared[:, 4 * lines :].reshape(
        2, row_groups, col_groups, n_rows // wide, TILE, wide, lane
    )
    inverse = inverse.transpose(0, 3, 5, 1, 4, 2, 6).reshape(2, width, width)

    def lower(panel, row):
        return jnp.where(row > panel, row_live[panel, row], 0).astype(jnp.float32)

    col_index = jnp.arange(matrix.shape[1] // width, dtype=jnp.int32) * n_cols + p

    def upper(panel):
        live = jnp.where(col_index > panel, jnp.take(col_live[panel], col_index), 0)
        return live.astype(jnp.float32)

    up0, up1 = upper(0), upper(1)
    both = matmul(jnp.concatenate([a_g0, a_10], axis=0), inverse[0])
    lower0 = both[:width] * lower(0, g)
    pivot_lower = both[width:] * lower(0, jnp.int32(1))
    a_g1 = a_g1 - matmul(lower0, a_01 * col_live[0, 1].astype(jnp.float32))
    lower1 = matmul(a_g1, inverse[1]) * lower(1, g)
    mixed = matmul(lower1, pivot_lower)

    left = jnp.stack(
        [
            jnp.concatenate([(lower0 - mixed * up1[j]) * up0[j], lower1 * up1[j]], axis=1)
            for j in range(matrix.shape[1] // width)
        ]
    )
    stored = jnp.where(p == 0, lower0, lower1)
    keeps = jnp.where(p == 0, g > 0, (p == 1) & (g > 1)).astype(jnp.int32).reshape(1)
    return update(keeps, matrix, raw, left, stored, length=width // n_rows)


def solution(mesh):
    in_specs = (P(ROWS, COLS), P(None, ROWS, None), P(), P())
    return jax.shard_map(
        per_device, mesh=mesh, in_specs=in_specs, out_specs=P(ROWS, COLS), check_vma=False
    )
```

```python
import functools

import jax
import jax.numpy as jnp
from jax import lax
from jax.experimental import pallas as pl
from jax.experimental.pallas import tpu as pltpu
from jax.sharding import PartitionSpec as P


ROWS, COLS = "prow", "pcol"
TILE = 8


def exchange(pieces, axis, groups=None):
    return lax.all_to_all(
        pieces, axis, split_axis=0, concat_axis=0, tiled=True, axis_index_groups=groups
    )


def copies(piece, count):
    return jnp.broadcast_to(piece, (count, *piece.shape))


def send_order(count):
    half = [d for i in range(1, count // 2) for d in (i, count - i)]
    return [*half, count // 2]


def scatter_rows(matrix):
    count, here = lax.axis_size(ROWS), lax.axis_index(ROWS)
    length = matrix.shape[0] // count
    turned = jnp.where(here == 1, jnp.roll(matrix, -length, axis=0), matrix)
    came = {}
    for d in send_order(count):
        pairs = [(0, d), (1, (1 + d) % count)]
        came[d] = lax.ppermute(turned[d * length : (d + 1) * length], ROWS, pairs)
    first = second = turned[:length]
    for d in came:
        first = jnp.where(here == d, came[d], first)
        second = jnp.where(here == (1 + d) % count, came[d], second)
    return jnp.concatenate([first, second], axis=0)


def tree_copies(own):
    count, here = lax.axis_size(ROWS), lax.axis_index(ROWS)
    held = own
    for c in range(4, count, 4):
        came = lax.ppermute(own, ROWS, [(0, c), (1, c + 1)])
        held = jnp.where((here == c) | (here == c + 1), came, held)
    leaves = [held]
    for step in (1, 2, -1):
        pairs = [((c + k) % count, (c + k + step) % count) for c in range(0, count, 4) for k in (0, 1)]
        leaves.append(lax.ppermute(held, ROWS, pairs))

    def of(place):
        found = leaves[0]
        for i in (1, 2, 3):
            found = jnp.where(place % 4 == i, leaves[i], found)
        return found

    return of(here), of(here + 3)


def plane(count):
    side = round((count // 2) ** 0.5)
    return side, lambda x, y, core: (x * side + y) * 2 + core


def holders(blocks):
    count = blocks.shape[0]
    side, _ = plane(count)
    grid = blocks.reshape(2, side, side, *blocks.shape[1:])
    both = jnp.stack([jnp.swapaxes(grid[0], 0, 1), grid[1]], axis=2)
    return both.reshape(blocks.shape)


def gather_plane(piece):
    count = lax.axis_size(COLS)
    side, at = plane(count)
    span = range(side)
    along_x = [[[at(x, y, c) for x in span] for y in span] for c in (0, 1)]
    along_y = [[[at(x, y, c) for y in span] for x in span] for c in (0, 1)]
    part = exchange(copies(piece, side), COLS, along_x[0] + along_y[1])
    part = exchange(copies(part, side), COLS, along_y[0] + along_x[1])
    part = part.reshape(side * side, *piece.shape)
    other = lax.ppermute(part, COLS, [(i, i ^ 1) for i in range(count)])
    return part, other


def halves(x):
    high = x.astype(jnp.bfloat16)
    return high, (x - high.astype(jnp.float32)).astype(jnp.bfloat16)


def product(left, right):
    dot = functools.partial(jnp.dot, preferred_element_type=jnp.float32)
    return dot(left[0], right[0]) + (dot(left[0], right[1]) + dot(left[1], right[0]))


def factors_kernel(lines, lane, n_rows, masks, part, other, high, low, stored, inverse):
    count, _, width = part.shape
    wide = width // lane
    blocks = [[] for _ in range(4)]
    for panel in (0, 1):
        source = jnp.where(masks[0] == panel, part[...], other[...])
        for i, block in enumerate(blocks):
            block.append(source[:, i * lines : (i + 1) * lines].reshape(count * lines, width))
        for t in range(count):
            for z in range(n_rows):
                row = z * (width // n_rows) + (t // wide) * TILE
                at = 4 * lines + (z // wide) * TILE
                inverse[panel, row : row + TILE, (t % wide) * lane : (t % wide + 1) * lane] = (
                    source[t, at : at + TILE, (z % wide) * lane : (z % wide + 1) * lane]
                )
    a_g0, a_g1, a_01, a_10 = (jnp.concatenate(block) for block in blocks)
    on = [masks[i].astype(jnp.float32) for i in range(10)]
    first = halves(inverse[0])
    lower0 = product(halves(a_g0), first) * on[1]
    pivot_lower = product(halves(a_10), first) * on[2]
    a_g1 = a_g1 - product(halves(lower0), halves(a_01 * on[3]))
    lower1 = product(halves(a_g1), halves(inverse[1])) * on[4]
    mixed = product(halves(lower1), halves(pivot_lower))
    stored[...] = jnp.where(masks[5] == 0, lower0, lower1)
    for j in (0, 1):
        high[j, :, :width], low[j, :, :width] = halves((lower0 - mixed * on[8 + j]) * on[6 + j])
        high[j, :, width:], low[j, :, width:] = halves(lower1 * on[8 + j])


def factors(masks, part, other, lines, lane, n_rows):
    width = part.shape[2]
    whole = pl.BlockSpec(memory_space=pltpu.VMEM)
    split = jax.ShapeDtypeStruct((2, width, 2 * width), jnp.bfloat16)
    return pl.pallas_call(
        functools.partial(factors_kernel, lines, lane, n_rows),
        in_specs=[pl.BlockSpec(memory_space=pltpu.SMEM), whole, whole],
        out_specs=[whole] * 3,
        out_shape=[split, split, jax.ShapeDtypeStruct((width, width), jnp.float32)],
        scratch_shapes=[pltpu.VMEM((2, width, width), jnp.float32)],
        cost_estimate=pl.CostEstimate(
            flops=30 * width**3, bytes_accessed=8 * part.size, transcendentals=0
        ),
        name="factors",
    )(masks, part, other)


def update_kernel(steps, length, keeps, matrix, raw, high, low, stored, out):
    rows = raw.shape[0]
    starts = [*range(0, rows, 2 * length), *range(length, rows, 2 * length)]
    split = [jnp.concatenate([x[i : i + length] for i in starts]) for x in halves(raw[...])]
    new = matrix[...] - product((high[0], low[0]), split)
    out[...] = jnp.where((keeps[0] == 1) & (pl.program_id(0) < steps), stored[...], new)


def update(keeps, matrix, raw, high, low, stored, length):
    rows, width = stored.shape
    cols = matrix.shape[1]
    wide = min(256, width)
    steps = width // wide
    factor = pl.BlockSpec((1, rows, 2 * rows), lambda t, _: (t // steps, 0, 0))
    return pl.pallas_call(
        functools.partial(update_kernel, steps, length),
        grid_spec=pltpu.PrefetchScalarGridSpec(
            num_scalar_prefetch=1,
            grid=(cols // wide,),
            in_specs=[
                pl.BlockSpec((rows, wide), lambda t, _: (0, t)),
                pl.BlockSpec((2 * rows, wide), lambda t, _: (0, t)),
                factor,
                factor,
                pl.BlockSpec((rows, wide), lambda t, _: (0, jnp.minimum(t, steps - 1))),
            ],
            out_specs=pl.BlockSpec((rows, wide), lambda t, _: (0, t)),
        ),
        out_shape=jax.ShapeDtypeStruct(matrix.shape, jnp.float32),
        cost_estimate=pl.CostEstimate(
            flops=12 * rows * rows * cols, bytes_accessed=32 * rows * cols, transcendentals=0
        ),
        name="update",
    )(keeps, matrix, raw, high, low, stored)


def per_device(matrix, pivot_inverse, row_live, col_live):
    width = pivot_inverse.shape[2]
    n_rows, n_cols = lax.axis_size(ROWS), lax.axis_size(COLS)
    g, p = lax.axis_index(ROWS), lax.axis_index(COLS)
    lines = width // n_cols
    lane = width * 2 * pivot_inverse.shape[1] // (TILE * n_cols)
    row_groups, col_groups = pivot_inverse.shape[1] // TILE, width // lane

    spread = exchange(holders(matrix[:, :width].reshape(n_cols, lines, width)), COLS)
    mine = spread[:2]

    pieces = scatter_rows(matrix)
    raw = lax.all_gather(pieces, ROWS, axis=0, tiled=True)

    cross = tree_copies(jnp.where(g == 0, mine[1], mine[0]))
    tiles = pivot_inverse.reshape(2, row_groups, TILE, col_groups, lane)
    tiles = tiles.transpose(0, 1, 3, 2, 4).reshape(n_cols, TILE, lane)
    tile = lax.dynamic_index_in_dim(holders(tiles), p, keepdims=False)
    pivots = exchange(copies(tile, n_rows), ROWS)
    wide = width // lane
    pivots = pivots.reshape(n_rows // wide, wide, TILE, lane)
    pivots = pivots.transpose(0, 2, 1, 3).reshape(-1, width)

    piece = jnp.concatenate([*mine, *cross, pivots], axis=0)
    part, other = gather_plane(piece)

    def lower(panel, row):
        return jnp.where(row > panel, row_live[panel, row], 0)

    col_index = jnp.arange(matrix.shape[1] // width, dtype=jnp.int32) * n_cols + p

    def upper(panel):
        return jnp.where(col_index > panel, jnp.take(col_live[panel], col_index), 0)

    scalars = jnp.stack([p % 2, lower(0, g), lower(0, jnp.int32(1)), col_live[0, 1], lower(1, g), p])
    masks = jnp.concatenate([scalars, upper(0), upper(1)])
    high, low, stored = factors(masks, part, other, lines=lines, lane=lane, n_rows=n_rows)
    keeps = jnp.where(p == 0, g > 0, (p == 1) & (g > 1)).astype(jnp.int32).reshape(1)
    return update(keeps, matrix, raw, high, low, stored, length=width // n_rows)


def solution(mesh):
    in_specs = (P(ROWS, COLS), P(None, ROWS, None), P(), P())
    return jax.shard_map(
        per_device, mesh=mesh, in_specs=in_specs, out_specs=P(ROWS, COLS), check_vma=False
    )
```

```python
import functools

import jax
import jax.numpy as jnp
from jax import lax
from jax.experimental import pallas as pl
from jax.experimental.pallas import tpu as pltpu
from jax.sharding import PartitionSpec as P


ROWS, COLS = "prow", "pcol"
TILE = 8


def exchange(pieces, axis, groups=None):
    return lax.all_to_all(
        pieces, axis, split_axis=0, concat_axis=0, tiled=True, axis_index_groups=groups
    )


def copies(piece, count):
    return jnp.broadcast_to(piece, (count, *piece.shape))


def send_order(count):
    half = [d for i in range(1, count // 2) for d in (i, count - i)]
    return [*half, count // 2]


def pick_kernel(length, *refs):
    *came, out, semaphores = refs
    count, here = len(came), lax.axis_index(ROWS)
    for panel in (0, 1):
        part = out.at[pl.ds(panel * length, length)]
        for d, source in enumerate(came):
            @pl.when(lax.rem(here + count - panel, count) == d)
            def _():
                pltpu.make_async_copy(source, part, semaphores.at[panel]).start()
    for panel in (0, 1):
        part = out.at[pl.ds(panel * length, length)]
        pltpu.make_async_copy(came[0], part, semaphores.at[panel]).wait()


def scatter_rows(matrix):
    count, here = lax.axis_size(ROWS), lax.axis_index(ROWS)
    length, cols = matrix.shape[0] // count, matrix.shape[1]
    turned = jnp.where(here == 1, jnp.roll(matrix, -length, axis=0), matrix)
    came = [turned[d * length : (d + 1) * length] for d in range(count)]
    for d in send_order(count):
        pairs = [(0, d), (1, (1 + d) % count)]
        came[d] = lax.ppermute(came[d], ROWS, pairs)
    return pl.pallas_call(
        functools.partial(pick_kernel, length),
        in_specs=[pl.BlockSpec(memory_space=pl.ANY)] * count,
        out_specs=pl.BlockSpec(memory_space=pltpu.VMEM),
        out_shape=jax.ShapeDtypeStruct((2 * length, cols), jnp.float32),
        scratch_shapes=[pltpu.SemaphoreType.DMA((2,))],
        cost_estimate=pl.CostEstimate(
            flops=matrix.size, bytes_accessed=16 * length * cols, transcendentals=0
        ),
        compiler_params=pltpu.CompilerParams(vmem_limit_bytes=4 * 2**20),
        name="pick",
    )(*came)


def tree_copies(own):
    count, here = lax.axis_size(ROWS), lax.axis_index(ROWS)
    held = own
    for c in range(4, count, 4):
        came = lax.ppermute(own, ROWS, [(0, c), (1, c + 1)])
        held = jnp.where((here == c) | (here == c + 1), came, held)
    leaves = [held]
    for step in (1, 2, -1):
        pairs = [((c + k) % count, (c + k + step) % count) for c in range(0, count, 4) for k in (0, 1)]
        leaves.append(lax.ppermute(held, ROWS, pairs))

    def of(place):
        found = leaves[0]
        for i in (1, 2, 3):
            found = jnp.where(place % 4 == i, leaves[i], found)
        return found

    return of(here), of(here + 3)


def plane(count):
    side = round((count // 2) ** 0.5)
    return side, lambda x, y, core: (x * side + y) * 2 + core


def holders(blocks):
    count = blocks.shape[0]
    side, _ = plane(count)
    grid = blocks.reshape(2, side, side, *blocks.shape[1:])
    both = jnp.stack([jnp.swapaxes(grid[0], 0, 1), grid[1]], axis=2)
    return both.reshape(blocks.shape)


def gather_plane(piece):
    count = lax.axis_size(COLS)
    side, at = plane(count)
    span = range(side)
    along_x = [[[at(x, y, c) for x in span] for y in span] for c in (0, 1)]
    along_y = [[[at(x, y, c) for y in span] for x in span] for c in (0, 1)]
    part = exchange(copies(piece, side), COLS, along_x[0] + along_y[1])
    part = exchange(copies(part, side), COLS, along_y[0] + along_x[1])
    part = part.reshape(side * side, *piece.shape)
    other = lax.ppermute(part, COLS, [(i, i ^ 1) for i in range(count)])
    return part, other


def halves(x):
    high = x.astype(jnp.bfloat16)
    return high, (x - high.astype(jnp.float32)).astype(jnp.bfloat16)


def product(left, right):
    dot = functools.partial(jnp.dot, preferred_element_type=jnp.float32)
    return dot(left[0], right[0]) + (dot(left[0], right[1]) + dot(left[1], right[0]))


def factors_kernel(lines, lane, n_rows, masks, part, other, high, low, stored, inverse):
    count, _, width = part.shape
    wide = width // lane
    blocks = [[] for _ in range(4)]
    for panel in (0, 1):
        source = jnp.where(masks[0] == panel, part[...], other[...])
        for i, block in enumerate(blocks):
            block.append(source[:, i * lines : (i + 1) * lines].reshape(count * lines, width))
        for t in range(count):
            for z in range(n_rows):
                row = z * (width // n_rows) + (t // wide) * TILE
                at = 4 * lines + (z // wide) * TILE
                inverse[panel, row : row + TILE, (t % wide) * lane : (t % wide + 1) * lane] = (
                    source[t, at : at + TILE, (z % wide) * lane : (z % wide + 1) * lane]
                )
    a_g0, a_g1, a_01, a_10 = (jnp.concatenate(block) for block in blocks)
    on = [masks[i].astype(jnp.float32) for i in range(10)]
    first = halves(inverse[0])
    lower0 = product(halves(a_g0), first) * on[1]
    pivot_lower = product(halves(a_10), first) * on[2]
    a_g1 = a_g1 - product(halves(lower0), halves(a_01 * on[3]))
    lower1 = product(halves(a_g1), halves(inverse[1])) * on[4]
    mixed = product(halves(lower1), halves(pivot_lower))
    stored[...] = jnp.where(masks[5] == 0, lower0, lower1)
    for j in (0, 1):
        high[j, :, :width], low[j, :, :width] = halves((lower0 - mixed * on[8 + j]) * on[6 + j])
        high[j, :, width:], low[j, :, width:] = halves(lower1 * on[8 + j])


def factors(masks, part, other, lines, lane, n_rows):
    width = part.shape[2]
    whole = pl.BlockSpec(memory_space=pltpu.VMEM)
    split = jax.ShapeDtypeStruct((2, width, 2 * width), jnp.bfloat16)
    return pl.pallas_call(
        functools.partial(factors_kernel, lines, lane, n_rows),
        in_specs=[pl.BlockSpec(memory_space=pltpu.SMEM), whole, whole],
        out_specs=[whole] * 3,
        out_shape=[split, split, jax.ShapeDtypeStruct((width, width), jnp.float32)],
        scratch_shapes=[pltpu.VMEM((2, width, width), jnp.float32)],
        cost_estimate=pl.CostEstimate(
            flops=30 * width**3, bytes_accessed=8 * part.size, transcendentals=0
        ),
        compiler_params=pltpu.CompilerParams(vmem_limit_bytes=36 * 2**20),
        name="factors",
    )(masks, part, other)


def update_kernel(steps, length, keeps, matrix, raw, high, low, stored, out):
    rows = raw.shape[0]
    starts = [*range(0, rows, 2 * length), *range(length, rows, 2 * length)]
    split = [jnp.concatenate([x[i : i + length] for i in starts]) for x in halves(raw[...])]
    block = pl.program_id(0) // steps
    new = matrix[...] - product((high[block], low[block]), split)
    out[...] = jnp.where((keeps[0] == 1) & (pl.program_id(0) < steps), stored[...], new)


def update(keeps, matrix, raw, high, low, stored, length):
    rows, width = stored.shape
    cols = matrix.shape[1]
    wide = min(256, width)
    steps = width // wide
    factor = pl.BlockSpec(memory_space=pltpu.VMEM)
    return pl.pallas_call(
        functools.partial(update_kernel, steps, length),
        grid_spec=pltpu.PrefetchScalarGridSpec(
            num_scalar_prefetch=1,
            grid=(cols // wide,),
            in_specs=[
                pl.BlockSpec((rows, wide), lambda t, _: (0, t)),
                pl.BlockSpec((2 * rows, wide), lambda t, _: (0, t)),
                factor,
                factor,
                pl.BlockSpec((rows, wide), lambda t, _: (0, jnp.minimum(t, steps - 1))),
            ],
            out_specs=pl.BlockSpec((rows, wide), lambda t, _: (0, t)),
        ),
        out_shape=jax.ShapeDtypeStruct(matrix.shape, jnp.float32),
        cost_estimate=pl.CostEstimate(
            flops=12 * rows * rows * cols, bytes_accessed=32 * rows * cols, transcendentals=0
        ),
        compiler_params=pltpu.CompilerParams(vmem_limit_bytes=54 * 2**20),
        name="update",
    )(keeps, matrix, raw, high, low, stored)


def per_device(matrix, pivot_inverse, row_live, col_live):
    width = pivot_inverse.shape[2]
    n_rows, n_cols = lax.axis_size(ROWS), lax.axis_size(COLS)
    g, p = lax.axis_index(ROWS), lax.axis_index(COLS)
    lines = width // n_cols
    lane = width * 2 * pivot_inverse.shape[1] // (TILE * n_cols)
    row_groups, col_groups = pivot_inverse.shape[1] // TILE, width // lane

    spread = exchange(holders(matrix[:, :width].reshape(n_cols, lines, width)), COLS)
    mine = spread[:2]

    pieces = scatter_rows(matrix)
    raw = lax.all_gather(pieces, ROWS, axis=0, tiled=True)

    cross = tree_copies(jnp.where(g == 0, mine[1], mine[0]))
    tiles = pivot_inverse.reshape(2, row_groups, TILE, col_groups, lane)
    tiles = tiles.transpose(0, 1, 3, 2, 4).reshape(n_cols, TILE, lane)
    tile = lax.dynamic_index_in_dim(holders(tiles), p, keepdims=False)
    pivots = exchange(copies(tile, n_rows), ROWS)
    wide = width // lane
    pivots = pivots.reshape(n_rows // wide, wide, TILE, lane)
    pivots = pivots.transpose(0, 2, 1, 3).reshape(-1, width)

    piece = jnp.concatenate([*mine, *cross, pivots], axis=0)
    part, other = gather_plane(piece)

    def lower(panel, row):
        return jnp.where(row > panel, row_live[panel, row], 0)

    col_index = jnp.arange(matrix.shape[1] // width, dtype=jnp.int32) * n_cols + p

    def upper(panel):
        return jnp.where(col_index > panel, jnp.take(col_live[panel], col_index), 0)

    scalars = jnp.stack([p % 2, lower(0, g), lower(0, jnp.int32(1)), col_live[0, 1], lower(1, g), p])
    masks = jnp.concatenate([scalars, upper(0), upper(1)])
    high, low, stored = factors(masks, part, other, lines=lines, lane=lane, n_rows=n_rows)
    keeps = jnp.where(p == 0, g > 0, (p == 1) & (g > 1)).astype(jnp.int32).reshape(1)
    return update(keeps, matrix, raw, high, low, stored, length=width // n_rows)


def solution(mesh):
    in_specs = (P(ROWS, COLS), P(None, ROWS, None), P(), P())
    return jax.shard_map(
        per_device, mesh=mesh, in_specs=in_specs, out_specs=P(ROWS, COLS), check_vma=False
    )
```
